32 devices in a mesh: left: 8 (over z, x), right: 4 (over y, core).
Axes of the slice: x: 2, y: 2, z: 4, core: 2. Of those that a mesh axis runs over, the one named last changes fastest.
Arguments:
- density: float32 [128, 128, 2048], P(None, 'left', 'right'), may hold values from -6 to 6
- symbol_x: float32 [128], replicated, may hold values from 0.3 to 3
- symbol_y: float32 [128], replicated, may hold values from 0.3 to 3
- symbol_z: float32 [2048], replicated, may hold values from 0.3 to 3
Outputs:
- spectrum: float32 [128, 128, 2048], P('left', 'right')
The draws below stay inside these ranges and needn't reach their ends.
All inputs are finite; a program needn't handle non-finite values.
Results may differ from the reference program's by a relative error of at most 0.00007.
Values sent between devices are 32-bit elements; how exact they have to be, the bound alone decides.
A program may use at most 192 MiB of HBM per device.

```python
import jax
import jax.numpy as jnp
from jax import lax

GRID_X = 128
GRID_Y = 128
GRID_Z = 2048


def level_of(rng, shape, split, smallest, high):
    def one(dim, parts):
        steps = jax.random.uniform(jax.random.fold_in(jax.random.fold_in(rng, 6), dim), (parts,), jnp.float32, smallest / len(split), high / len(split))
        return jnp.repeat(jnp.exp(steps), shape[dim] // parts).reshape((-1,) + (1,) * (len(shape) - dim - 1))

    level = one(*split[0])
    for cut in split[1:]:
        level = level * one(*cut)
    return level


def centred(key, shape, scale, most, pieces=(), kind=jnp.bfloat16):
    level = level_of(key, shape, pieces, -0.22, 0.18) if pieces else 1.0
    array = jax.random.normal(key, shape, jnp.float32) * scale * level
    return jnp.minimum(jnp.maximum(array, -most), most).astype(kind)


def setup_inputs(seed: int = 0) -> dict:
    streams_of = jax.random.split(jax.random.key(seed), 5)
    density = centred(streams_of[0], (GRID_X, GRID_Y, GRID_Z), 1.0, 6.0, ((1, 8), (2, 4)), jnp.float32)
    symbol_x = jnp.clip(jax.random.uniform(streams_of[1], (GRID_X,), jnp.float32, 0.3, 3.0), 0.3, 3.0)
    symbol_y = jnp.clip(jax.random.uniform(streams_of[2], (GRID_Y,), jnp.float32, 0.3, 3.0), 0.3, 3.0)
    symbol_z = jnp.clip(jax.random.uniform(streams_of[3], (GRID_Z,), jnp.float32, 0.3, 3.0), 0.3, 3.0)
    return {"density": density, "symbol_x": symbol_x, "symbol_y": symbol_y, "symbol_z": symbol_z}


def mode_table(count):
    rank = jnp.arange(count)
    angle = 2.0 * jnp.pi / count * (rank[:, None] * rank[None, :] % count).astype(jnp.float32)
    return (jnp.cos(angle) + jnp.sin(angle)) * count ** (-0.5)

def transform_dim(values, dim):
    moved = jnp.tensordot(values, mode_table(values.shape[dim]), axes=([dim], [0]), precision=lax.Precision.HIGHEST)
    return jnp.moveaxis(moved, -1, dim)

def reference(density, symbol_x, symbol_y, symbol_z):
    spectrum = density
    spectrum = transform_dim(spectrum, 0)
    spectrum = transform_dim(spectrum, 1)
    spectrum = transform_dim(spectrum, 2)
    symbol = symbol_x[:, None, None] + symbol_y[None, :, None] + symbol_z[None, None, :]
    spectrum = spectrum * lax.rsqrt(symbol)
    return spectrum
```

```python
import functools

import jax
import jax.numpy as jnp
import numpy as np
from jax import lax
from jax.experimental import pallas as pl
from jax.experimental.pallas import tpu as pltpu
from jax.sharding import PartitionSpec as P

LANES = 128
VMEM_BYTES = 60 * 2**20
MESH = pl.DeviceIdType.MESH
F32 = jnp.float32
BF16 = jnp.bfloat16


def mode_table(count):
    rank = jnp.arange(count)
    angle = 2.0 * jnp.pi / count * (rank[:, None] * rank[None, :] % count).astype(jnp.float32)
    return (jnp.cos(angle) + jnp.sin(angle)) * count ** (-0.5)


def transform_dim(values, dim):
    moved = jnp.tensordot(
        values, mode_table(values.shape[dim]), axes=([dim], [0]), precision=lax.Precision.HIGHEST
    )
    return jnp.moveaxis(moved, -1, dim)


def exchange_plain(density):
    values = transform_dim(density, 0)
    values = lax.all_to_all(values, "left", split_axis=0, concat_axis=1, tiled=True)
    values = transform_dim(values, 1)
    values = lax.all_to_all(values, "right", split_axis=1, concat_axis=2, tiled=True)
    return transform_dim(values, 2)


def numpy_angles(rows, count):
    return 2.0 * np.pi / count * (np.outer(rows, np.arange(count)) % count)


def two_parts(table):
    high = np.asarray(table, np.float32).astype(BF16)
    low = (table - high.astype(np.float64)).astype(np.float32).astype(BF16)
    return np.stack([high, low])


def small_table(count):
    angles = numpy_angles(np.arange(count), count)
    return two_parts((np.cos(angles) + np.sin(angles)) * count**-0.5)


def seeds(count, fine):
    coarse_angles = numpy_angles(np.arange(count // fine) * fine, count)
    coarse = np.stack([np.cos(coarse_angles), np.sin(coarse_angles)])
    fine_angles = numpy_angles(np.arange(fine), count)
    cosine, sine = np.cos(fine_angles), np.sin(fine_angles)
    return coarse.astype(np.float32), (np.stack([cosine + sine, cosine - sine]) * count**-0.5).astype(np.float32)


def split(values):
    high = values.astype(BF16)
    return high, (values - high.astype(F32)).astype(BF16)


def dot(a, b):
    return jnp.dot(a, b, preferred_element_type=F32)


def dot_three(a_high, a_low, b_high, b_low):
    return dot(a_high, b_high) + (dot(a_low, b_high) + dot(a_high, b_low))


def kernel(dims, density, table_x, table_y, coarse, fine, out, entry, send1, recv1, send2, recv2, table_high,
           table_low, part_high, part_low, total, in_sem, out_sem, s1_sem, r1_sem, s2_sem, r2_sem):
    X, Y, Z, L, R, Xl, Yl, Yr, Zl, C, zc, fine_rows = dims
    left, right = lax.axis_index("left"), lax.axis_index("right")

    def in_copy(c):
        return pltpu.make_async_copy(density.at[:, pl.ds(c * zc, zc)], entry.at[c], in_sem.at[c])

    for c in range(C):
        in_copy(c).start()

    def partner(index, step, count):
        if count & (count - 1) == 0:
            return index ^ step
        return lax.rem(index + step, count)

    def source(index, step, count):
        if count & (count - 1) == 0:
            return index ^ step
        return lax.rem(index + count - step, count)

    barrier = pltpu.get_barrier_semaphore()
    for step in range(1, L):
        pl.semaphore_signal(barrier, inc=1, device_id=(partner(left, step, L), right), device_id_type=MESH)
    for step in range(1, R):
        pl.semaphore_signal(barrier, inc=1, device_id=(left, partner(right, step, R)), device_id_type=MESH)
    pl.semaphore_wait(barrier, L + R - 2)

    def copy1(c, step):
        to = partner(left, step, L)
        return pltpu.make_async_remote_copy(
            src_ref=send1.at[c, pl.ds(to * Xl, Xl)],
            dst_ref=recv1.at[c, :, pl.ds(pl.multiple_of(left * Yl, 8), Yl), :],
            send_sem=s1_sem.at[c, step],
            recv_sem=r1_sem.at[c, step],
            device_id=(to, right),
            device_id_type=MESH,
        )

    def copy2(c, step):
        to = partner(right, step, R)
        return pltpu.make_async_remote_copy(
            src_ref=send2.at[c, :, pl.ds(pl.multiple_of(to * Yr, 8), Yr), :],
            dst_ref=recv2.at[c, :, :, pl.ds(pl.multiple_of(right * zc, LANES), zc)],
            send_sem=s2_sem.at[c, step],
            recv_sem=r2_sem.at[c, step],
            device_id=(left, to),
            device_id_type=MESH,
        )

    group = 4

    def first(c):
        in_copy(c).wait()
        high, low = table_x[0], table_x[1]
        target = send1.at[c].reshape(X * Yl, zc)

        def body(g, _):
            lines = [entry[c, pl.ds(g * group + j, X, stride=Yl), :] for j in range(group)]
            b_high, b_low = split(jnp.concatenate(lines, axis=1))
            moved = dot_three(high, low, b_high, b_low)
            for j in range(group):
                target[pl.ds(g * group + j, X, stride=Yl), :] = moved[:, j * zc:(j + 1) * zc]
            return 0

        lax.fori_loop(0, Yl // group, body, 0)
        for step in range(1, L):
            copy1(c, step).start()
        recv1[c, :, pl.ds(pl.multiple_of(left * Yl, 8), Yl), :] = send1[c, pl.ds(left * Xl, Xl)]

    def second(c):
        for step in range(1, L):
            copy1(c, step).wait_recv()
        high, low = table_y[0], table_y[1]

        def body(g, _):
            lines = [recv1[c, g * group + j] for j in range(group)]
            b_high, b_low = split(jnp.concatenate(lines, axis=1))
            moved = dot_three(high, low, b_high, b_low)
            for j in range(group):
                send2[c, g * group + j] = moved[:, j * zc:(j + 1) * zc]
            return 0

        lax.fori_loop(0, Xl // group, body, 0)
        for step in range(1, R):
            copy2(c, step).start()
        recv2[c, :, :, pl.ds(pl.multiple_of(right * zc, LANES), zc)] = send2[
            c, :, pl.ds(pl.multiple_of(right * Yr, 8), Yr), :]

    rows = Xl * Yr
    wide = 512

    def third(c):
        for step in range(1, R):
            copy2(c, step).wait_recv()

        def split_body(x, _):
            high, low = split(recv2[c, x])
            at = pl.ds(pl.multiple_of(x * Yr, 16), Yr)
            part_high[at, :] = high
            part_low[at, :] = low
            return 0

        lax.fori_loop(0, Xl, split_body, 0)

        def body(n, _):
            at = pl.ds(pl.multiple_of(n * wide, LANES), wide)
            term = dot_three(part_high[...], part_low[...], table_high[c, :, at], table_low[c, :, at])
            if c > 0:
                term = total[:, at] + term
            total[:, at] = term
            if c == C - 1:
                pltpu.make_async_copy(total.at[:, at], out.at[:, at], out_sem.at[n]).start()
            return 0

        lax.fori_loop(0, Z // wide, body, 0)

    def tables(c):
        per = zc // fine_rows

        def body(i, _):
            base = lax.div(i, per) * (Zl // fine_rows) + c * per + lax.rem(i, per)
            cosine, sine = coarse[0, pl.ds(base, 1), :], coarse[1, pl.ds(base, 1), :]

            def inner(q, _):
                at = pl.ds(pl.multiple_of(q * 16, 16), 16)
                high, low = split(cosine * fine[0, at, :] + sine * fine[1, at, :])
                to = pl.ds(pl.multiple_of(i * fine_rows + q * 16, 16), 16)
                table_high[c, to, :] = high
                table_low[c, to, :] = low
                return 0

            return lax.fori_loop(0, fine_rows // 16, inner, 0)

        lax.fori_loop(0, R * per, body, 0)

    for c in range(C):
        first(c)
    for c in range(C):
        tables(c)
    for c in range(C):
        second(c)
        if c > 0:
            third(c - 1)
    third(C - 1)

    for n in range(Z // wide):
        at = pl.ds(n * wide, wide)
        pltpu.make_async_copy(total.at[:, at], out.at[:, at], out_sem.at[n]).wait()
    for c in range(C):
        for step in range(1, L):
            copy1(c, step).wait_send()
        for step in range(1, R):
            copy2(c, step).wait_send()


def exchange_kernel(density, L, R, fine_rows, Z):
    X, Yl, Zl = density.shape
    Y, Xl = Yl * L, X // L
    Yr, zc = Y // R, LANES
    C = Zl // zc
    dims = (X, Y, Z, L, R, Xl, Yl, Yr, Zl, C, zc, fine_rows)
    coarse, fine = seeds(Z, fine_rows)
    vmem = pl.BlockSpec(memory_space=pltpu.VMEM)
    hbm = pl.BlockSpec(memory_space=pl.ANY)
    dma = pltpu.SemaphoreType.DMA
    flat = pl.pallas_call(
        functools.partial(kernel, dims),
        out_shape=jax.ShapeDtypeStruct((Xl * Yr, Z), F32),
        in_specs=[hbm, vmem, vmem, vmem, vmem],
        out_specs=hbm,
        scratch_shapes=[
            pltpu.VMEM((C, X * Yl, zc), F32),
            pltpu.VMEM((C, X, Yl, zc), F32),
            pltpu.VMEM((C, Xl, Y, zc), F32),
            pltpu.VMEM((C, Xl, Y, zc), F32),
            pltpu.VMEM((C, Xl, Yr, R * zc), F32),
            pltpu.VMEM((C, R * zc, Z), BF16),
            pltpu.VMEM((C, R * zc, Z), BF16),
            pltpu.VMEM((Xl * Yr, R * zc), BF16),
            pltpu.VMEM((Xl * Yr, R * zc), BF16),
            pltpu.VMEM((Xl * Yr, Z), F32),
            dma((C,)),
            dma((Z // 512,)),
            dma((C, L)),
            dma((C, L)),
            dma((C, R)),
            dma((C, R)),
        ],
        compiler_params=pltpu.CompilerParams(
            collective_id=0, has_side_effects=True, vmem_limit_bytes=VMEM_BYTES
        ),
    )(density.reshape(X * Yl, Zl), small_table(X), small_table(Y), coarse, fine)
    return flat.reshape(Xl, Yr, Z)


def per_device(L, R, density, symbol_x, symbol_y, symbol_z):
    X, Yl, Zl = density.shape
    Z = Zl * R
    fine_rows = 64
    held = 6 * density.size * 4 + 2 * Z * Z * 2 + 2 * (Z // fine_rows + fine_rows) * Z * 4 + 8 * 2**20
    fits = (held <= VMEM_BYTES and Zl % LANES == 0 and Z % 512 == 0 and Yl % 8 == 0 and X % (4 * L) == 0
            and Yl * L % (16 * R) == 0)
    block_values = exchange_kernel(density, L, R, fine_rows, Z) if fits else exchange_plain(density)
    share_x = block_values.shape[0]
    part_x = lax.dynamic_slice_in_dim(symbol_x, lax.axis_index("left") * share_x, share_x)
    share_y = block_values.shape[1]
    part_y = lax.dynamic_slice_in_dim(symbol_y, lax.axis_index("right") * share_y, share_y)
    symbol = part_x[:, None, None] + part_y[None, :, None] + symbol_z[None, None, :]
    return block_values * lax.rsqrt(symbol)


def solution(mesh):
    return jax.shard_map(
        functools.partial(per_device, mesh.shape["left"], mesh.shape["right"]),
        mesh=mesh,
        in_specs=(P(None, "left", "right"), P(), P(), P()),
        out_specs=P("left", "right", None),
        check_vma=False,
    )
```

```python
import functools

import jax
import jax.numpy as jnp
import numpy as np
from jax import lax
from jax.experimental import pallas as pl
from jax.experimental.pallas import tpu as pltpu
from jax.sharding import PartitionSpec as P

LANES = 128
VMEM_BYTES = 60 * 2**20
MESH = pl.DeviceIdType.MESH
F32 = jnp.float32
BF16 = jnp.bfloat16


def mode_table(count):
    rank = jnp.arange(count)
    angle = 2.0 * jnp.pi / count * (rank[:, None] * rank[None, :] % count).astype(jnp.float32)
    return (jnp.cos(angle) + jnp.sin(angle)) * count ** (-0.5)


def transform_dim(values, dim):
    moved = jnp.tensordot(
        values, mode_table(values.shape[dim]), axes=([dim], [0]), precision=lax.Precision.HIGHEST
    )
    return jnp.moveaxis(moved, -1, dim)


def exchange_plain(density):
    values = transform_dim(density, 0)
    values = lax.all_to_all(values, "left", split_axis=0, concat_axis=1, tiled=True)
    values = transform_dim(values, 1)
    values = lax.all_to_all(values, "right", split_axis=1, concat_axis=2, tiled=True)
    return transform_dim(values, 2)


def numpy_angles(rows, count):
    return 2.0 * np.pi / count * (np.outer(rows, np.arange(count)) % count)


def two_parts(table):
    high = np.asarray(table, np.float32).astype(BF16)
    low = (table - high.astype(np.float64)).astype(np.float32).astype(BF16)
    return np.stack([high, low])


def small_table(count):
    angles = numpy_angles(np.arange(count), count)
    return two_parts((np.cos(angles) + np.sin(angles)) * count**-0.5)


def seeds(count, fine):
    coarse_angles = numpy_angles(np.arange(count // fine) * fine, count)
    coarse = np.stack([np.cos(coarse_angles), np.sin(coarse_angles)])
    fine_angles = numpy_angles(np.arange(fine), count)
    cosine, sine = np.cos(fine_angles), np.sin(fine_angles)
    return coarse.astype(np.float32), (np.stack([cosine + sine, cosine - sine]) * count**-0.5).astype(np.float32)


def split(values):
    high = values.astype(BF16)
    return high, (values - high.astype(F32)).astype(BF16)


def dot(a, b):
    return jnp.dot(a, b, preferred_element_type=F32)


def dot_three(a_high, a_low, b_high, b_low):
    return dot(a_high, b_high) + (dot(a_low, b_high) + dot(a_high, b_low))


def kernel(dims, parts, density, table_x, table_y, coarse_in, fine_in, symbol_x, symbol_y, symbol_z, out, entry,
           send1, recv1, send2, recv2, table_high, table_low, part_high, part_low, total, scale, coarse, fine,
           in_sem, seed_sem, out_sem, s1_sem, r1_sem, s2_sem, r2_sem):
    X, Y, Z, L, R, Xl, Yl, Yr, Zl, C, zc, fine_rows = dims
    left, right = lax.axis_index("left"), lax.axis_index("right")

    def in_copy(c):
        return pltpu.make_async_copy(density.at[:, pl.ds(c * zc, zc)], entry.at[c], in_sem.at[c])

    seed_copies = [
        pltpu.make_async_copy(coarse_in, coarse, seed_sem.at[0]),
        pltpu.make_async_copy(fine_in, fine, seed_sem.at[1]),
    ]

    def partner(index, step, count):
        if count & (count - 1) == 0:
            return index ^ step
        return lax.rem(index + step, count)

    barrier = pltpu.get_barrier_semaphore()
    for step in range(1, L):
        pl.semaphore_signal(barrier, inc=1, device_id=(partner(left, step, L), right), device_id_type=MESH)
    for step in range(1, R):
        pl.semaphore_signal(barrier, inc=1, device_id=(left, partner(right, step, R)), device_id_type=MESH)
    for c in range(C):
        in_copy(c).start()
    for copy in seed_copies:
        copy.start()

    def copy1(p, step):
        c, x0, xn = parts[p]
        to = partner(left, step, L)
        return pltpu.make_async_remote_copy(
            src_ref=send1.at[c, pl.ds(to * Xl + x0, xn)],
            dst_ref=recv1.at[c, pl.ds(x0, xn), pl.ds(pl.multiple_of(left * Yl, 8), Yl), :],
            send_sem=s1_sem.at[p, step],
            recv_sem=r1_sem.at[p, step],
            device_id=(to, right),
            device_id_type=MESH,
        )

    def copy2(p, step):
        c, x0, xn = parts[p]
        to = partner(right, step, R)
        return pltpu.make_async_remote_copy(
            src_ref=send2.at[c, pl.ds(x0, xn), pl.ds(pl.multiple_of(to * Yr, 8), Yr), :],
            dst_ref=recv2.at[c, pl.ds(x0, xn), :, pl.ds(pl.multiple_of(right * zc, LANES), zc)],
            send_sem=s2_sem.at[p, step],
            recv_sem=r2_sem.at[p, step],
            device_id=(left, to),
            device_id_type=MESH,
        )

    group = 4
    wide = 512

    def first(c):
        in_copy(c).wait()
        high, low = table_x[0], table_x[1]
        target = send1.at[c].reshape(X * Yl, zc)

        def body(g, _):
            lines = [entry[c, pl.ds(g * group + j, X, stride=Yl), :] for j in range(group)]
            b_high, b_low = split(jnp.concatenate(lines, axis=1))
            moved = dot_three(high, low, b_high, b_low)
            for j in range(group):
                target[pl.ds(g * group + j, X, stride=Yl), :] = moved[:, j * zc:(j + 1) * zc]
            return 0

        lax.fori_loop(0, Yl // group, body, 0)

    def first_send(c):
        for p, part in enumerate(parts):
            if part[0] == c:
                for step in range(1, L):
                    copy1(p, step).start()
        recv1[c, :, pl.ds(pl.multiple_of(left * Yl, 8), Yl), :] = send1[c, pl.ds(left * Xl, Xl)]

    def second(p):
        c, x0, xn = parts[p]
        for step in range(1, L):
            copy1(p, step).wait_recv()
        high, low = table_y[0], table_y[1]
        lot = min(group, xn)

        def body(g, _):
            x = x0 + g * lot
            lines = [recv1[c, x + j] for j in range(lot)]
            b_high, b_low = split(jnp.concatenate(lines, axis=1))
            moved = dot_three(high, low, b_high, b_low)
            for j in range(lot):
                send2[c, x + j] = moved[:, j * zc:(j + 1) * zc]
            return 0

        lax.fori_loop(0, xn // lot, body, 0)
        for step in range(1, R):
            copy2(p, step).start()
        recv2[c, pl.ds(x0, xn), :, pl.ds(pl.multiple_of(right * zc, LANES), zc)] = send2[
            c, pl.ds(x0, xn), pl.ds(pl.multiple_of(right * Yr, 8), Yr), :]

    def out_copy(p, n):
        c, x0, xn = parts[p]
        rows, at = pl.ds(x0 * Yr, xn * Yr), pl.ds(pl.multiple_of(n * wide, LANES), wide)
        return pltpu.make_async_copy(total.at[rows, at], out.at[rows, at], out_sem.at[p, n])

    def third(p):
        c, x0, xn = parts[p]
        for step in range(1, R):
            copy2(p, step).wait_recv()

        def split_body(x, _):
            high, low = split(recv2[c, x])
            at = pl.ds(pl.multiple_of(x * Yr, 16), Yr)
            part_high[at, :] = high
            part_low[at, :] = low
            return 0

        lax.fori_loop(x0, x0 + xn, split_body, 0)
        rows = pl.ds(x0 * Yr, xn * Yr)

        def body(n, _):
            at = pl.ds(pl.multiple_of(n * wide, LANES), wide)
            term = dot_three(part_high[rows, :], part_low[rows, :], table_high[c, :, at], table_low[c, :, at])
            if c > 0:
                term = total[rows, at] + term
            if c == C - 1:
                term = term * scale[rows, at]
            total[rows, at] = term
            if c == C - 1:
                out_copy(p, n).start()
            return 0

        lax.fori_loop(0, Z // wide, body, 0)

    def tables(c):
        per = zc // fine_rows

        def body(i, _):
            base = lax.div(i, per) * (Zl // fine_rows) + c * per + lax.rem(i, per)
            cosine, sine = coarse[0, pl.ds(base, 1), :], coarse[1, pl.ds(base, 1), :]

            def inner(q, _):
                at = pl.ds(pl.multiple_of(q * 16, 16), 16)
                high, low = split(cosine * fine[0, at, :] + sine * fine[1, at, :])
                to = pl.ds(pl.multiple_of(i * fine_rows + q * 16, 16), 16)
                table_high[c, to, :] = high
                table_low[c, to, :] = low
                return 0

            return lax.fori_loop(0, fine_rows // 16, inner, 0)

        lax.fori_loop(0, R * per, body, 0)

    def scales():
        line = lax.broadcasted_iota(jnp.int32, (Yr, LANES), 0)
        column = jnp.zeros((Yr, LANES), F32)
        for j in range(Yr):
            column = jnp.where(line == j, symbol_y[right * Yr + j], column)

        def body(x, _):
            start = column + symbol_x[left * Xl + x]
            rows = pl.ds(pl.multiple_of(x * Yr, 8), Yr)
            for k in range(0, Z, LANES):
                scale[rows, k:k + LANES] = lax.rsqrt(start + symbol_z[:, k:k + LANES])
            return 0

        lax.fori_loop(0, Xl, body, 0)

    first(0)
    pl.semaphore_wait(barrier, L + R - 2)
    first_send(0)
    for c in range(1, C):
        first(c)
        first_send(c)
    for copy in seed_copies:
        copy.wait()
    for c in range(C):
        tables(c)
    scales()
    for p in range(len(parts)):
        second(p)
        if p > 0:
            third(p - 1)
    third(len(parts) - 1)

    for p, part in enumerate(parts):
        if part[0] == C - 1:
            for n in range(Z // wide):
                out_copy(p, n).wait()
    for p in range(len(parts)):
        for step in range(1, L):
            copy1(p, step).wait_send()
        for step in range(1, R):
            copy2(p, step).wait_send()


CUTS = (1, 2, 2, 4)


def exchange_kernel(density, symbol_x, symbol_y, symbol_z, L, R, fine_rows):
    X, Yl, Zl = density.shape
    Y, Xl, Z = Yl * L, X // L, Zl * R
    Yr, zc = Y // R, LANES
    C = Zl // zc
    dims = (X, Y, Z, L, R, Xl, Yl, Yr, Zl, C, zc, fine_rows)
    cuts = [1] * (C - len(CUTS)) + list(CUTS[-C:])
    parts = [(c, i * (Xl // cuts[c]), Xl // cuts[c]) for c in range(C) for i in range(cuts[c])]
    coarse, fine = seeds(Z, fine_rows)
    vmem = pl.BlockSpec(memory_space=pltpu.VMEM)
    smem = pl.BlockSpec(memory_space=pltpu.SMEM)
    hbm = pl.BlockSpec(memory_space=pl.ANY)
    dma = pltpu.SemaphoreType.DMA
    flat = pl.pallas_call(
        functools.partial(kernel, dims, parts),
        out_shape=jax.ShapeDtypeStruct((Xl * Yr, Z), F32),
        in_specs=[hbm, vmem, vmem, hbm, hbm, smem, smem, vmem],
        out_specs=hbm,
        scratch_shapes=[
            pltpu.VMEM((C, X * Yl, zc), F32),
            pltpu.VMEM((C, X, Yl, zc), F32),
            pltpu.VMEM((C, Xl, Y, zc), F32),
            pltpu.VMEM((C, Xl, Y, zc), F32),
            pltpu.VMEM((C, Xl, Yr, R * zc), F32),
            pltpu.VMEM((C, R * zc, Z), BF16),
            pltpu.VMEM((C, R * zc, Z), BF16),
            pltpu.VMEM((Xl * Yr, R * zc), BF16),
            pltpu.VMEM((Xl * Yr, R * zc), BF16),
            pltpu.VMEM((Xl * Yr, Z), F32),
            pltpu.VMEM((Xl * Yr, Z), F32),
            pltpu.VMEM(coarse.shape, F32),
            pltpu.VMEM(fine.shape, F32),
            dma((C,)),
            dma((2,)),
            dma((len(parts), Z // 512)),
            dma((len(parts), L)),
            dma((len(parts), L)),
            dma((len(parts), R)),
            dma((len(parts), R)),
        ],
        compiler_params=pltpu.CompilerParams(
            collective_id=0, has_side_effects=True, vmem_limit_bytes=VMEM_BYTES
        ),
    )(density.reshape(X * Yl, Zl), small_table(X), small_table(Y), coarse, fine, symbol_x, symbol_y,
      symbol_z.reshape(1, Z))
    return flat.reshape(Xl, Yr, Z)


def per_device(L, R, density, symbol_x, symbol_y, symbol_z):
    X, Yl, Zl = density.shape
    Z = Zl * R
    fine_rows = 64
    held = 7 * density.size * 4 + 2 * Z * Z * 2 + 2 * (Z // fine_rows + fine_rows) * Z * 4 + 4 * 2**20
    fits = (held <= VMEM_BYTES and Zl % LANES == 0 and Z % 512 == 0 and Yl % 8 == 0 and X % (16 * L) == 0
            and Yl * L % (16 * R) == 0)
    if fits:
        return exchange_kernel(density, symbol_x, symbol_y, symbol_z, L, R, fine_rows)
    block_values = exchange_plain(density)
    share_x = block_values.shape[0]
    part_x = lax.dynamic_slice_in_dim(symbol_x, lax.axis_index("left") * share_x, share_x)
    share_y = block_values.shape[1]
    part_y = lax.dynamic_slice_in_dim(symbol_y, lax.axis_index("right") * share_y, share_y)
    symbol = part_x[:, None, None] + part_y[None, :, None] + symbol_z[None, None, :]
    return block_values * lax.rsqrt(symbol)


def solution(mesh):
    return jax.shard_map(
        functools.partial(per_device, mesh.shape["left"], mesh.shape["right"]),
        mesh=mesh,
        in_specs=(P(None, "left", "right"), P(), P(), P()),
        out_specs=P("left", "right", None),
        check_vma=False,
    )
```

```python
import functools

import jax
import jax.numpy as jnp
import numpy as np
from jax import lax
from jax.experimental import pallas as pl
from jax.experimental.pallas import tpu as pltpu
from jax.sharding import PartitionSpec as P

LANES = 128
VMEM_BYTES = 60 * 2**20
MESH = pl.DeviceIdType.MESH
F32 = jnp.float32
BF16 = jnp.bfloat16


def mode_table(count):
    rank = jnp.arange(count)
    angle = 2.0 * jnp.pi / count * (rank[:, None] * rank[None, :] % count).astype(jnp.float32)
    return (jnp.cos(angle) + jnp.sin(angle)) * count ** (-0.5)


def transform_dim(values, dim):
    moved = jnp.tensordot(
        values, mode_table(values.shape[dim]), axes=([dim], [0]), precision=lax.Precision.HIGHEST
    )
    return jnp.moveaxis(moved, -1, dim)


def exchange_plain(density):
    values = transform_dim(density, 0)
    values = lax.all_to_all(values, "left", split_axis=0, concat_axis=1, tiled=True)
    values = transform_dim(values, 1)
    values = lax.all_to_all(values, "right", split_axis=1, concat_axis=2, tiled=True)
    return transform_dim(values, 2)


def numpy_angles(rows, count):
    return 2.0 * np.pi / count * (np.outer(rows, np.arange(count)) % count)


def two_parts(table):
    high = np.asarray(table, np.float32).astype(BF16)
    low = (table - high.astype(np.float64)).astype(np.float32).astype(BF16)
    return np.stack([high, low])


def small_table(count):
    angles = numpy_angles(np.arange(count), count)
    return two_parts((np.cos(angles) + np.sin(angles)) * count**-0.5)


def seeds(count, fine):
    coarse_angles = numpy_angles(np.arange(count // fine) * fine, count)
    coarse = np.stack([np.cos(coarse_angles), np.sin(coarse_angles)])
    fine_angles = numpy_angles(np.arange(fine), count)
    cosine, sine = np.cos(fine_angles), np.sin(fine_angles)
    return coarse.astype(np.float32), (np.stack([cosine + sine, cosine - sine]) * count**-0.5).astype(np.float32)


def split(values):
    high = values.astype(BF16)
    return high, (values - high.astype(F32)).astype(BF16)


def dot(a, b):
    return jnp.dot(a, b, preferred_element_type=F32)


def dot_three(a_high, a_low, b_high, b_low):
    return dot(a_high, b_high) + (dot(a_low, b_high) + dot(a_high, b_low))


def kernel(dims, parts, density, table_x, table_y, coarse_in, fine_in, symbol_x, symbol_y, symbol_z, out, entry,
           send1, recv1, send2, recv2, table_high, table_low, part_high, part_low, total, scale, coarse, fine,
           in_sem, seed_sem, out_sem, s1_sem, r1_sem, s2_sem, r2_sem):
    X, Y, Z, L, R, Xl, Yl, Yr, Zl, C, zc, fine_rows = dims
    left, right = lax.axis_index("left"), lax.axis_index("right")

    def in_copy(c):
        return pltpu.make_async_copy(density.at[:, pl.ds(c * zc, zc)], entry.at[c], in_sem.at[c])

    seed_copies = [
        pltpu.make_async_copy(coarse_in, coarse, seed_sem.at[0]),
        pltpu.make_async_copy(fine_in, fine, seed_sem.at[1]),
    ]

    def partner(index, step, count):
        if count & (count - 1) == 0:
            return index ^ step
        return lax.rem(index + step, count)

    barrier = pltpu.get_barrier_semaphore()
    for step in range(1, L):
        pl.semaphore_signal(barrier, inc=1, device_id=(partner(left, step, L), right), device_id_type=MESH)
    for step in range(1, R):
        pl.semaphore_signal(barrier, inc=1, device_id=(left, partner(right, step, R)), device_id_type=MESH)
    for c in range(C):
        in_copy(c).start()
    for copy in seed_copies:
        copy.start()

    def copy1(p, step):
        c, x0, xn = parts[p]
        to = partner(left, step, L)
        return pltpu.make_async_remote_copy(
            src_ref=send1.at[c, pl.ds(to * Xl + x0, xn)],
            dst_ref=recv1.at[c, pl.ds(x0, xn), pl.ds(pl.multiple_of(left * Yl, 8), Yl), :],
            send_sem=s1_sem.at[p, step],
            recv_sem=r1_sem.at[p, step],
            device_id=(to, right),
            device_id_type=MESH,
        )

    def copy2(p, step):
        c, x0, xn = parts[p]
        to = partner(right, step, R)
        return pltpu.make_async_remote_copy(
            src_ref=send2.at[c, pl.ds(x0, xn), pl.ds(pl.multiple_of(to * Yr, 8), Yr), :],
            dst_ref=recv2.at[c, pl.ds(x0, xn), :, pl.ds(pl.multiple_of(right * zc, LANES), zc)],
            send_sem=s2_sem.at[p, step],
            recv_sem=r2_sem.at[p, step],
            device_id=(left, to),
            device_id_type=MESH,
        )

    group = 4
    wide = 512

    def first(c):
        in_copy(c).wait()
        high, low = table_x[0], table_x[1]
        target = send1.at[c].reshape(X * Yl, zc)

        def body(g, _):
            lines = [entry[c, pl.ds(g * group + j, X, stride=Yl), :] for j in range(group)]
            b_high, b_low = split(jnp.concatenate(lines, axis=1))
            moved = dot_three(high, low, b_high, b_low)
            for j in range(group):
                target[pl.ds(g * group + j, X, stride=Yl), :] = moved[:, j * zc:(j + 1) * zc]
            return 0

        lax.fori_loop(0, Yl // group, body, 0)

    def first_send(c):
        for p, part in enumerate(parts):
            if part[0] == c:
                for step in range(1, L):
                    copy1(p, step).start()
        recv1[c, :, pl.ds(pl.multiple_of(left * Yl, 8), Yl), :] = send1[c, pl.ds(left * Xl, Xl)]

    def second(p):
        c, x0, xn = parts[p]
        for step in range(1, L):
            copy1(p, step).wait_recv()
        high, low = table_y[0], table_y[1]
        lot = min(group, xn)

        def body(g, _):
            x = x0 + g * lot
            lines = [recv1[c, x + j] for j in range(lot)]
            b_high, b_low = split(jnp.concatenate(lines, axis=1))
            moved = dot_three(high, low, b_high, b_low)
            for j in range(lot):
                send2[c, x + j] = moved[:, j * zc:(j + 1) * zc]
            return 0

        lax.fori_loop(0, xn // lot, body, 0)
        for step in range(1, R):
            copy2(p, step).start()
        recv2[c, pl.ds(x0, xn), :, pl.ds(pl.multiple_of(right * zc, LANES), zc)] = send2[
            c, pl.ds(x0, xn), pl.ds(pl.multiple_of(right * Yr, 8), Yr), :]

    def out_copy(p, n):
        c, x0, xn = parts[p]
        rows, at = pl.ds(x0 * Yr, xn * Yr), pl.ds(pl.multiple_of(n * wide, LANES), wide)
        return pltpu.make_async_copy(total.at[rows, at], out.at[rows, at], out_sem.at[p, n])

    def third(p):
        c, x0, xn = parts[p]
        for step in range(1, R):
            copy2(p, step).wait_recv()

        def split_body(x, _):
            high, low = split(recv2[c, x])
            at = pl.ds(pl.multiple_of(x * Yr, 16), Yr)
            part_high[at, :] = high
            part_low[at, :] = low
            return 0

        lax.fori_loop(x0, x0 + xn, split_body, 0)
        rows = pl.ds(x0 * Yr, xn * Yr)

        def body(n, _):
            at = pl.ds(pl.multiple_of(n * wide, LANES), wide)
            term = dot_three(part_high[rows, :], part_low[rows, :], table_high[c, :, at], table_low[c, :, at])
            if c > 0:
                term = total[rows, at] + term
            if c == C - 1:
                term = term * scale[rows, at]
            total[rows, at] = term
            if c == C - 1:
                out_copy(p, n).start()
            return 0

        lax.fori_loop(0, Z // wide, body, 0)

    def tables(c):
        per = zc // fine_rows

        def body(i, _):
            base = lax.div(i, per) * (Zl // fine_rows) + c * per + lax.rem(i, per)
            cosine, sine = coarse[0, pl.ds(base, 1), :], coarse[1, pl.ds(base, 1), :]

            def inner(q, _):
                at = pl.ds(pl.multiple_of(q * 16, 16), 16)
                high, low = split(cosine * fine[0, at, :] + sine * fine[1, at, :])
                to = pl.ds(pl.multiple_of(i * fine_rows + q * 16, 16), 16)
                table_high[c, to, :] = high
                table_low[c, to, :] = low
                return 0

            return lax.fori_loop(0, fine_rows // 16, inner, 0)

        lax.fori_loop(0, R * per, body, 0)

    def scales():
        line = lax.broadcasted_iota(jnp.int32, (Yr, LANES), 0)
        column = jnp.zeros((Yr, LANES), F32)
        for j in range(Yr):
            column = jnp.where(line == j, symbol_y[right * Yr + j], column)

        def body(x, _):
            start = column + symbol_x[left * Xl + x]
            rows = pl.ds(pl.multiple_of(x * Yr, 8), Yr)
            for k in range(0, Z, LANES):
                scale[rows, k:k + LANES] = lax.rsqrt(start + symbol_z[:, k:k + LANES])
            return 0

        lax.fori_loop(0, Xl, body, 0)

    first(0)
    pl.semaphore_wait(barrier, L + R - 2)
    first_send(0)
    for c in range(1, C):
        first(c)
        first_send(c)
    for copy in seed_copies:
        copy.wait()
    for c in range(C):
        tables(c)
    scales()
    done = 0
    for p, part in enumerate(parts):
        second(p)
        if part[0] < C - 1 and p > 0:
            third(done)
            done += 1
    for p in range(done, len(parts)):
        third(p)

    for p, part in enumerate(parts):
        if part[0] == C - 1:
            for n in range(Z // wide):
                out_copy(p, n).wait()
    for p in range(len(parts)):
        for step in range(1, L):
            copy1(p, step).wait_send()
        for step in range(1, R):
            copy2(p, step).wait_send()


CUTS = (1, 2, 2, 4)


def exchange_kernel(density, symbol_x, symbol_y, symbol_z, L, R, fine_rows):
    X, Yl, Zl = density.shape
    Y, Xl, Z = Yl * L, X // L, Zl * R
    Yr, zc = Y // R, LANES
    C = Zl // zc
    dims = (X, Y, Z, L, R, Xl, Yl, Yr, Zl, C, zc, fine_rows)
    cuts = [1] * (C - len(CUTS)) + list(CUTS[-C:])
    parts = [(c, i * (Xl // cuts[c]), Xl // cuts[c]) for c in range(C) for i in range(cuts[c])]
    coarse, fine = seeds(Z, fine_rows)
    vmem = pl.BlockSpec(memory_space=pltpu.VMEM)
    smem = pl.BlockSpec(memory_space=pltpu.SMEM)
    hbm = pl.BlockSpec(memory_space=pl.ANY)
    dma = pltpu.SemaphoreType.DMA
    flat = pl.pallas_call(
        functools.partial(kernel, dims, parts),
        out_shape=jax.ShapeDtypeStruct((Xl * Yr, Z), F32),
        in_specs=[hbm, vmem, vmem, hbm, hbm, smem, smem, vmem],
        out_specs=hbm,
        scratch_shapes=[
            pltpu.VMEM((C, X * Yl, zc), F32),
            pltpu.VMEM((C, X, Yl, zc), F32),
            pltpu.VMEM((C, Xl, Y, zc), F32),
            pltpu.VMEM((C, Xl, Y, zc), F32),
            pltpu.VMEM((C, Xl, Yr, R * zc), F32),
            pltpu.VMEM((C, R * zc, Z), BF16),
            pltpu.VMEM((C, R * zc, Z), BF16),
            pltpu.VMEM((Xl * Yr, R * zc), BF16),
            pltpu.VMEM((Xl * Yr, R * zc), BF16),
            pltpu.VMEM((Xl * Yr, Z), F32),
            pltpu.VMEM((Xl * Yr, Z), F32),
            pltpu.VMEM(coarse.shape, F32),
            pltpu.VMEM(fine.shape, F32),
            dma((C,)),
            dma((2,)),
            dma((len(parts), Z // 512)),
            dma((len(parts), L)),
            dma((len(parts), L)),
            dma((len(parts), R)),
            dma((len(parts), R)),
        ],
        compiler_params=pltpu.CompilerParams(
            collective_id=0, has_side_effects=True, vmem_limit_bytes=VMEM_BYTES
        ),
    )(density.reshape(X * Yl, Zl), small_table(X), small_table(Y), coarse, fine, symbol_x, symbol_y,
      symbol_z.reshape(1, Z))
    return flat.reshape(Xl, Yr, Z)


def per_device(L, R, density, symbol_x, symbol_y, symbol_z):
    X, Yl, Zl = density.shape
    Z = Zl * R
    fine_rows = 64
    held = 7 * density.size * 4 + 2 * Z * Z * 2 + 2 * (Z // fine_rows + fine_rows) * Z * 4 + 4 * 2**20
    fits = (held <= VMEM_BYTES and Zl % LANES == 0 and Z % 512 == 0 and Yl % 8 == 0 and X % (16 * L) == 0
            and Yl * L % (16 * R) == 0)
    if fits:
        return exchange_kernel(density, symbol_x, symbol_y, symbol_z, L, R, fine_rows)
    block_values = exchange_plain(density)
    share_x = block_values.shape[0]
    part_x = lax.dynamic_slice_in_dim(symbol_x, lax.axis_index("left") * share_x, share_x)
    share_y = block_values.shape[1]
    part_y = lax.dynamic_slice_in_dim(symbol_y, lax.axis_index("right") * share_y, share_y)
    symbol = part_x[:, None, None] + part_y[None, :, None] + symbol_z[None, None, :]
    return block_values * lax.rsqrt(symbol)


def solution(mesh):
    return jax.shard_map(
        functools.partial(per_device, mesh.shape["left"], mesh.shape["right"]),
        mesh=mesh,
        in_specs=(P(None, "left", "right"), P(), P(), P()),
        out_specs=P("left", "right", None),
        check_vma=False,
    )
```
